32 devices in a mesh: cfg: 2 (over x), seq: 16 (over z, y, core).
Axes of the slice: x: 2, y: 2, z: 4, core: 2. Of those that a mesh axis runs over, the one named last changes fastest.
Arguments:
- latent: bfloat16 [16, 1024, 1536], P('seq'), may hold values from -6 to 6
- text_ids: int32 [2, 512], P('cfg'), may hold values from 0 to 32127
- timestep: int32 [1], replicated, may hold values from 0 to 999
- guide_num: int32 [1], replicated, may hold values from 1024 to 8192
- guide_den: int32 [1], replicated, may hold values from 512 to 1024
- text_table: bfloat16 [32128, 1536], P('seq'), may hold values from -6 to 6
- time_in: bfloat16 [256, 1536], replicated, may hold values from -0.375 to 0.375
- time_out: bfloat16 [1536, 1536], P(None, 'seq'), may hold values from -0.15625 to 0.15625
- mod_weight: bfloat16 [1536, 7680], P(None, 'seq'), may hold values from -0.109375 to 0.109375
- qkv_weight: bfloat16 [1536, 4608], replicated, may hold values from -1 to 1
- out_weight: bfloat16 [1536, 1536], replicated, may hold values from -0.625 to 0.625
- head_weight: bfloat16 [1536, 64], replicated, may hold values from -0.15625 to 0.15625
Outputs:
- guided: float32 [16, 1024, 64], P('seq')
The draws below stay inside these ranges and needn't reach their ends.
All inputs are finite; a program needn't handle non-finite values.
Results may differ from the reference program's by a relative error of at most 0.0117.
Values may be sent and summed in bfloat16 or wider, within the bound.
A program may use at most 128 MiB of HBM per device.

```python
import math
import jax
import jax.numpy as jnp
import numpy as np
from jax import lax

D = 1536
HEADS = 24
OUT_CH = 64
VOCAB = 32128
FREQ = 256
TEXT = 512
PIXELS = 1024
FRAMES = 16
N_SEQ = 16


def draw_qkv_weight(key, part):
    base_key, head_key = jax.random.split(jax.random.fold_in(key, 17))
    spread_scale = 1.0 / math.sqrt(D)
    entries = jax.random.truncated_normal(base_key, -4.0, 4.0, (D, 3 * D), jnp.float32) * spread_scale
    return jnp.clip(entries, -1.0, 1.0).astype(jnp.bfloat16)


def touch_ends(result, stream_key, least, top_value):
    longest = result.shape.index(max(result.shape))
    spots = []
    for shift in (0, 1):
        where = [jax.random.randint(jax.random.fold_in(stream_key, axis), (), 0, length) for axis, length in enumerate(result.shape)]
        where[longest] = (where[longest] + shift) % result.shape[longest]
        spots.append(tuple(where))
    return result.at[spots[0]].set(least).at[spots[1]].set(top_value)


def block_levels(stream_key, dims, cuts, low, high):
    def one(dim, parts):
        heights = jax.random.uniform(jax.random.fold_in(jax.random.fold_in(stream_key, 6), dim), (parts,), jnp.float32, low / len(cuts), high / len(cuts))
        return jnp.repeat(jnp.exp(heights), dims[dim] // parts).reshape((-1,) + (1,) * (len(dims) - dim - 1))

    loudness = one(*cuts[0])
    for cut in cuts[1:]:
        loudness = loudness * one(*cut)
    return loudness


def rank_table(amount, skew):
    weights = [(1 << 20) // math.isqrt(rank ** skew) + 1 for rank in range(1, amount + 1)]
    width = 1 + sum(weights) // (1 << 30)
    return np.cumsum(np.array([max(1, weight // width) for weight in weights]))


def ranked(stream_key, dims, count, skew):
    table = rank_table(count, skew)
    pick = jax.random.randint(jax.random.fold_in(stream_key, 1), dims, 0, int(table[count - 1]))
    rank = jnp.searchsorted(jnp.asarray(table, jnp.int32), pick, side="right")
    return jax.random.permutation(jax.random.fold_in(stream_key, 2), count)[rank].astype(jnp.int32)


def scatter_about(rng, shape, scale, reach, shards=(), kind=jnp.bfloat16):
    drawn = jax.random.normal(rng, shape, jnp.float32) * scale
    if len(shards) > 0:
        drawn = block_levels(rng, shape, shards, -0.22, 0.18) * drawn
    return jnp.clip(drawn, min=-reach, max=reach).astype(kind)


def setup_inputs(seed: int = 0) -> dict:
    seeds = jax.random.split(jax.random.key(seed), 13)
    return {
        "latent": scatter_about(seeds[0], (FRAMES, PIXELS, D), 1.0, 6.0, ((0, 16),)),
        "text_ids": touch_ends(ranked(seeds[1], (2, TEXT), VOCAB, 1), jax.random.fold_in(seeds[1], 3), 0, VOCAB - 1).astype(jnp.int32),
        "timestep": jax.random.randint(seeds[2], (1,), 0, 1000).astype(jnp.int32),
        "guide_num": jax.random.randint(seeds[3], (1,), 1024, 8193).astype(jnp.int32),
        "guide_den": jax.random.randint(seeds[4], (1,), 512, 1025).astype(jnp.int32),
        "text_table": scatter_about(seeds[5], (VOCAB, D), 1.0, 6.0, ((0, 16),)),
        "time_in": scatter_about(seeds[6], (FREQ, D), FREQ ** -0.5, 0.375),
        "time_out": scatter_about(seeds[7], (D, D), D ** -0.5, 0.15625, ((1, 16),)),
        "mod_weight": scatter_about(seeds[8], (D, 5 * D), (2 * D) ** -0.5, 0.109375, ((1, 16),)),
        "qkv_weight": draw_qkv_weight(jax.random.fold_in(seeds[12], 71), 0),
        "out_weight": scatter_about(seeds[10], (D, D), (D // 16) ** -0.5, 0.625),
        "head_weight": scatter_about(seeds[11], (D, OUT_CH), D ** -0.5, 0.15625),
    }


norm_floor = 0.1

def layer_norm(values):
    center = values - lax.optimization_barrier(jnp.mean(values, axis=-1, keepdims=True))
    spread = lax.optimization_barrier(jnp.mean(center * center, axis=-1, keepdims=True))
    return center * lax.rsqrt(spread + norm_floor)

def modulate(values, shift_part, scale_part):
    return (layer_norm(values) * (1.0 + scale_part) + shift_part).astype(jnp.bfloat16)

def time_features(timestep):
    half_width = FREQ // 2
    ladder = jnp.arange(half_width, dtype=jnp.float32)
    freq_rates = jnp.exp(-math.log(10000.0) * ladder / half_width)
    angles = timestep.astype(jnp.float32)[0] * freq_rates
    return jnp.concatenate([jnp.cos(angles), jnp.sin(angles)])[None, :].astype(jnp.bfloat16)

def temporal_mix(normed, qkv_weight):
    frame_count, item_count, model_width = normed.shape
    head_dim = model_width // HEADS
    projected = jnp.dot(normed.reshape(-1, model_width), qkv_weight, preferred_element_type=jnp.float32)
    qkv_parts = []
    for part_index in range(3):
        rounded = projected[:, part_index * model_width:(part_index + 1) * model_width].astype(jnp.bfloat16)
        rounded = lax.optimization_barrier(rounded)
        qkv_parts.append(rounded.astype(jnp.float32).reshape(frame_count, item_count, HEADS, head_dim))
    scores = jnp.einsum('fphd,gphd->phfg', qkv_parts[0], qkv_parts[1]) * (1.0 / math.sqrt(head_dim))
    attn_prob = lax.optimization_barrier(jax.nn.softmax(scores, axis=-1).astype(jnp.bfloat16))
    mixed_rows = jnp.einsum('phfg,gphd->fphd', attn_prob.astype(jnp.float32), qkv_parts[2])
    return mixed_rows.astype(jnp.bfloat16).reshape(frame_count, item_count, model_width)

def finish_tokens(latent_part, mixed_rows, out_weight, head_weight, gate_attn, shift_out, scale_out):
    model_width = latent_part.shape[-1]
    base_rows = latent_part.reshape(-1, model_width).astype(jnp.float32)
    branch = jnp.dot(mixed_rows.reshape(-1, model_width), out_weight, preferred_element_type=jnp.float32)
    residual = base_rows + gate_attn * branch
    final_in = modulate(residual, shift_out, scale_out)
    prediction = jnp.dot(final_in, head_weight, preferred_element_type=jnp.float32)
    return prediction.reshape(latent_part.shape[:-1] + (head_weight.shape[1],))

def block_pass(latent_block, modulation, qkv_weight, out_weight, head_weight):
    shift_attn, scale_attn, gate_attn, shift_out, scale_out = jnp.split(modulation, 5)
    normed = modulate(latent_block.astype(jnp.float32), shift_attn, scale_attn)
    mixed_rows = temporal_mix(normed, qkv_weight)
    return finish_tokens(latent_block, mixed_rows, out_weight, head_weight, gate_attn, shift_out, scale_out)

def reference(latent, text_ids, timestep, guide_num, guide_den, text_table, time_in, time_out, mod_weight, qkv_weight, out_weight, head_weight):
    time_hidden = jax.nn.silu(jnp.dot(time_features(timestep), time_in, preferred_element_type=jnp.float32)).astype(jnp.bfloat16)
    time_embed = jnp.dot(time_hidden, time_out, preferred_element_type=jnp.float32)[0]
    blocks = PIXELS // N_SEQ
    by_block = jnp.transpose(latent.reshape(FRAMES, N_SEQ, blocks, D), (1, 0, 2, 3))
    predictions = []
    for pass_index in range(2):
        ids_row = text_ids[pass_index]
        pooled = lax.optimization_barrier(jnp.sum(jnp.take(text_table, ids_row, axis=0).astype(jnp.float32), axis=0)) / jnp.sqrt(jnp.float32(TEXT))
        cond_vec = jax.nn.silu(time_embed + pooled).astype(jnp.bfloat16)
        modulation = jnp.dot(cond_vec[None, :], mod_weight, preferred_element_type=jnp.float32)[0]

        def run_block(latent_block):
            return block_pass(latent_block, modulation, qkv_weight, out_weight, head_weight)
        prediction = lax.map(run_block, by_block)
        predictions.append(jnp.transpose(prediction, (1, 0, 2, 3)).reshape(FRAMES, PIXELS, OUT_CH))
    guide_scale = guide_num[0].astype(jnp.float32) / guide_den[0].astype(jnp.float32)
    return predictions[1] + guide_scale * (predictions[0] - predictions[1])
```

```python
import functools
import math

import jax
import jax.numpy as jnp
from jax import lax
from jax.experimental import pallas as pl
from jax.experimental.pallas import tpu as pltpu
from jax.sharding import PartitionSpec as P

HEADS = 24
FREQ = 256
NORM_FLOOR = 0.1
GROUP = 8
VMEM_BYTES = 60 * 1024 * 1024
MESH = pl.DeviceIdType.MESH


def layer_norm(values):
    center = values - jnp.mean(values, axis=-1, keepdims=True)
    spread = jnp.mean(center * center, axis=-1, keepdims=True)
    return center * lax.rsqrt(spread + NORM_FLOOR)


def time_features(timestep):
    half_width = FREQ // 2
    ladder = jnp.arange(half_width, dtype=jnp.float32)
    freq_rates = jnp.exp(-math.log(10000.0) * ladder / half_width)
    angles = timestep.astype(jnp.float32)[0] * freq_rates
    return jnp.concatenate([jnp.cos(angles), jnp.sin(angles)])[None, :].astype(jnp.bfloat16)


def pool_kernel(ids_ref, placed_ref, table_ref, out_ref, counts_ref):
    rows = table_ref.shape[0]
    tokens = ids_ref.shape[0]

    @pl.when(pl.program_id(0) == 0)
    def _():
        lanes = lax.broadcasted_iota(jnp.int32, (tokens, rows), 1)
        hits = jnp.where(ids_ref[...] == lanes, 1.0, 0.0)
        counts = jnp.sum(hits, axis=0, keepdims=True)
        high = jnp.floor(counts * (1.0 / 256.0)) * 256.0
        counts_ref[...] = jnp.concatenate([high, counts - high], axis=0)

    sums = jnp.dot(
        counts_ref[...].astype(jnp.bfloat16), table_ref[...], preferred_element_type=jnp.float32
    )
    total = jnp.sum(sums, axis=0, keepdims=True)
    out_ref[...] = total * (1.0 / math.sqrt(tokens)) + placed_ref[...]


def pool(ids_local, placed, table):
    voc, width = table.shape
    cols = width // 3
    return pl.pallas_call(
        pool_kernel,
        grid=(3,),
        out_shape=jax.ShapeDtypeStruct((1, width), jnp.float32),
        in_specs=[
            pl.BlockSpec(ids_local.shape, lambda j: (0, 0)),
            pl.BlockSpec((1, cols), lambda j: (0, j)),
            pl.BlockSpec((voc, cols), lambda j: (0, j)),
        ],
        out_specs=pl.BlockSpec((1, cols), lambda j: (0, j)),
        scratch_shapes=[pltpu.VMEM((2, voc), jnp.float32)],
        compiler_params=pltpu.CompilerParams(vmem_limit_bytes=VMEM_BYTES),
        name="pool",
    )(ids_local, placed, table)


def greet_all(n_cfg, n_seq):
    cfg, me = lax.axis_index("cfg"), lax.axis_index("seq")
    barrier = pltpu.get_barrier_semaphore()
    total = n_cfg * n_seq

    def hello(k, carry):
        flat = lax.rem(cfg * n_seq + me + k, total)
        pl.semaphore_signal(
            barrier, inc=1, device_id=(flat // n_seq, lax.rem(flat, n_seq)), device_id_type=MESH
        )
        return carry

    lax.fori_loop(1, total, hello, 0)
    pl.semaphore_wait(barrier, total - 1)


def exchange_kernel(
    n_cfg, n_seq, msg_ref, latent_ref, mod_w_ref, got_ref, mod_ref,
    slots, mods, part, own, msg_send, msg_recv, lat_send, lat_recv, mod_send, mod_recv, own_sem,
):
    cfg, me = lax.axis_index("cfg"), lax.axis_index("seq")
    total = n_cfg * n_seq
    mine = cfg * n_seq + me
    frames, pixels, _ = latent_ref.shape
    half = pixels // n_cfg
    items = half // n_seq

    greet_all(n_cfg, n_seq)

    def piece(owner):
        start = pl.multiple_of(cfg * half + owner * items, items)
        return latent_ref.at[:, pl.ds(start, items), :]

    def msg_copy(k):
        flat = lax.rem(mine + k, total)
        return pltpu.make_async_remote_copy(
            src_ref=msg_ref, dst_ref=slots.at[mine], send_sem=msg_send.at[k],
            recv_sem=msg_recv.at[k],
            device_id=(flat // n_seq, lax.rem(flat, n_seq)), device_id_type=MESH,
        )

    def lat_copy(k):
        peer = lax.rem(me + k, n_seq)
        return pltpu.make_async_remote_copy(
            src_ref=piece(peer), dst_ref=got_ref.at[pl.ds(me * frames, frames)],
            send_sem=lat_send.at[k], recv_sem=lat_recv.at[k],
            device_id=(cfg, peer), device_id_type=MESH,
        )

    def mod_copy(k):
        peer = lax.rem(me + k, n_seq)
        return pltpu.make_async_remote_copy(
            src_ref=part, dst_ref=mods.at[me], send_sem=mod_send.at[k], recv_sem=mod_recv.at[k],
            device_id=(cfg, peer), device_id_type=MESH,
        )

    def start_msg(k, carry):
        msg_copy(k).start()
        return carry

    def start_lat(k, carry):
        lat_copy(k).start()
        return carry

    def start_mod(k, carry):
        mod_copy(k).start()
        return carry

    def end_msg(k, carry):
        msg_copy(k).wait()
        return carry

    def end_lat(k, carry):
        lat_copy(k).wait()
        return carry

    def end_mod(k, carry):
        mod_copy(k).wait()
        return carry

    own_in = pltpu.make_async_copy(piece(me), own, own_sem.at[0])
    own_out = pltpu.make_async_copy(own, got_ref.at[pl.ds(me * frames, frames)], own_sem.at[1])
    lax.fori_loop(1, total, start_msg, 0)
    own_in.start()
    lax.fori_loop(1, n_seq, start_lat, 0)
    slots[mine] = msg_ref[...]
    own_in.wait()
    own_out.start()
    lax.fori_loop(1, total, end_msg, 0)
    rows = []
    for c in range(n_cfg):
        rows.append(jnp.sum(slots[c * n_seq : (c + 1) * n_seq], axis=0))
    cond = jnp.concatenate(rows, axis=0)
    cond = (cond / (1.0 + jnp.exp(-cond))).astype(jnp.bfloat16)
    mod_part = jnp.dot(cond, mod_w_ref[...], preferred_element_type=jnp.float32)
    part[...] = mod_part
    mods[me] = mod_part
    lax.fori_loop(1, n_seq, start_mod, 0)
    own_out.wait()
    lax.fori_loop(1, n_seq, end_mod, 0)
    mod_ref[...] = mods[...]
    lax.fori_loop(1, n_seq, end_lat, 0)


def exchange(n_cfg, n_seq, msg, latent, mod_weight):
    frames, pixels, width = latent.shape
    items = pixels // n_cfg // n_seq
    cols = mod_weight.shape[1]
    vmem = pl.BlockSpec(memory_space=pltpu.VMEM)
    hbm = pl.BlockSpec(memory_space=pl.ANY)
    total = n_cfg * n_seq
    return pl.pallas_call(
        functools.partial(exchange_kernel, n_cfg, n_seq),
        out_shape=(
            jax.ShapeDtypeStruct((n_seq * frames, items, width), jnp.bfloat16),
            jax.ShapeDtypeStruct((n_seq, n_cfg, cols), jnp.float32),
        ),
        in_specs=[vmem, hbm, vmem],
        out_specs=(hbm, vmem),
        scratch_shapes=[
            pltpu.VMEM((total, 1, width), jnp.float32),
            pltpu.VMEM((n_seq, n_cfg, cols), jnp.float32),
            pltpu.VMEM((n_cfg, cols), jnp.float32),
            pltpu.VMEM((frames, items, width), jnp.bfloat16),
            pltpu.SemaphoreType.DMA((total,)),
            pltpu.SemaphoreType.DMA((total,)),
            pltpu.SemaphoreType.DMA((n_seq,)),
            pltpu.SemaphoreType.DMA((n_seq,)),
            pltpu.SemaphoreType.DMA((n_seq,)),
            pltpu.SemaphoreType.DMA((n_seq,)),
            pltpu.SemaphoreType.DMA((2,)),
        ],
        compiler_params=pltpu.CompilerParams(
            collective_id=0, has_side_effects=True, vmem_limit_bytes=VMEM_BYTES
        ),
        name="exchange",
    )(msg, latent, mod_weight)


def block_kernel(
    head_dim, scale_ref, lat_ref, mod_ref, wq_ref, wk_ref, wv_ref, wo_hbm, wh_ref, out_ref,
    base, normed, qs, ks, vs, mixed, wo, wo_sem,
):
    step = pl.program_id(0)
    frames, items, width = lat_ref.shape
    groups = items // GROUP
    rows = frames * GROUP
    tokens = groups * rows
    cols = wq_ref.shape[1]
    pair = 2 * head_dim
    wo_copy = pltpu.make_async_copy(wo_hbm, wo, wo_sem)

    @pl.when(step == 0)
    def _():
        wo_copy.start()
        values = lat_ref[...].astype(jnp.float32)
        for g in range(groups):
            x = values[:, g * GROUP : (g + 1) * GROUP, :].reshape(rows, width)
            base[g * rows : (g + 1) * rows, :] = x.astype(jnp.bfloat16)
            n = layer_norm(x)
            for c in range(2):
                y = n * (1.0 + mod_ref[c, 1:2, :]) + mod_ref[c, 0:1, :]
                at = c * tokens + g * rows
                normed[at : at + rows, :] = y.astype(jnp.bfloat16)

    lane = lax.broadcasted_iota(jnp.int32, (1, pair), 1)
    left = jnp.where(lane < head_dim, 1.0, 0.0).astype(jnp.bfloat16)
    right = jnp.where(lane < head_dim, 0.0, 1.0).astype(jnp.bfloat16)
    same = lax.broadcasted_iota(jnp.int32, (1, GROUP, rows), 1) == lax.rem(
        lax.broadcasted_iota(jnp.int32, (1, GROUP, rows), 2), GROUP
    )
    for c in range(2):
        span = slice(c * tokens, (c + 1) * tokens)
        x = normed[span, :]
        q = jnp.dot(x, wq_ref[...], preferred_element_type=jnp.float32)
        qs[span, :] = (q * (1.0 / math.sqrt(head_dim))).astype(jnp.bfloat16)
        k = jnp.dot(x, wk_ref[...], preferred_element_type=jnp.float32)
        ks[span, :] = k.astype(jnp.bfloat16)
        v = jnp.dot(x, wv_ref[...], preferred_element_type=jnp.float32)
        vs[span, :] = v.astype(jnp.bfloat16)
        for g in range(groups):
            at = slice(c * tokens + g * rows, c * tokens + (g + 1) * rows)
            for h in range(cols // pair):
                lanes = slice(h * pair, (h + 1) * pair)
                kk = ks[at, lanes]
                vv = vs[at, lanes]
                keys = jnp.concatenate([kk * left, kk * right], axis=0)
                vals = jnp.concatenate([vv * left, vv * right], axis=0)
                scores = lax.dot_general(
                    keys, qs[at, lanes], (((1,), (1,)), ((), ())),
                    preferred_element_type=jnp.float32,
                )
                probs = []
                for s in range(2):
                    t = scores[s * rows : (s + 1) * rows].reshape(frames, GROUP, rows)
                    e = jnp.exp(t - jnp.max(t, axis=0, keepdims=True))
                    r = jnp.where(same, 1.0 / jnp.sum(e, axis=0, keepdims=True), 0.0)
                    probs.append((e * r).reshape(rows, rows))
                prob = jnp.concatenate(probs, axis=0).astype(jnp.bfloat16)
                o = lax.dot_general(
                    prob, vals, (((0,), (0,)), ((), ())), preferred_element_type=jnp.float32
                )
                mixed[step, at, lanes] = o.astype(jnp.bfloat16)

    @pl.when(step == pl.num_programs(0) - 1)
    def _():
        wo_copy.wait()
        steps = width // cols
        preds = []
        for c in range(2):
            span = slice(c * tokens, (c + 1) * tokens)
            full = jnp.concatenate([mixed[j, span, :] for j in range(steps)], axis=1)
            branch = jnp.dot(full, wo[...], preferred_element_type=jnp.float32)
            residual = base[...].astype(jnp.float32) + mod_ref[c, 2:3, :] * branch
            final = layer_norm(residual) * (1.0 + mod_ref[c, 4:5, :]) + mod_ref[c, 3:4, :]
            preds.append(
                jnp.dot(
                    final.astype(jnp.bfloat16), wh_ref[...], preferred_element_type=jnp.float32
                )
            )
        guided = preds[1] + scale_ref[0, 0] * (preds[0] - preds[1])
        for g in range(groups):
            out_ref[:, g * GROUP : (g + 1) * GROUP, :] = guided[g * rows : (g + 1) * rows].reshape(
                frames, GROUP, guided.shape[1]
            )


def block(scale, lat, mod, qkv_weight, out_weight, head_weight):
    frames, items, width = lat.shape
    head_dim = width // HEADS
    cols = 4 * head_dim
    steps = width // cols
    tokens = frames * items
    out_ch = head_weight.shape[1]
    return pl.pallas_call(
        functools.partial(block_kernel, head_dim),
        grid=(steps,),
        out_shape=jax.ShapeDtypeStruct((frames, items, out_ch), jnp.float32),
        in_specs=[
            pl.BlockSpec(memory_space=pltpu.SMEM),
            pl.BlockSpec(lat.shape, lambda j: (0, 0, 0)),
            pl.BlockSpec(mod.shape, lambda j: (0, 0, 0)),
            pl.BlockSpec((width, cols), lambda j: (0, j)),
            pl.BlockSpec((width, cols), lambda j: (0, steps + j)),
            pl.BlockSpec((width, cols), lambda j: (0, 2 * steps + j)),
            pl.BlockSpec(memory_space=pl.ANY),
            pl.BlockSpec(head_weight.shape, lambda j: (0, 0)),
        ],
        out_specs=pl.BlockSpec((frames, items, out_ch), lambda j: (0, 0, 0)),
        scratch_shapes=[
            pltpu.VMEM((tokens, width), jnp.bfloat16),
            pltpu.VMEM((2 * tokens, width), jnp.bfloat16),
            pltpu.VMEM((2 * tokens, cols), jnp.bfloat16),
            pltpu.VMEM((2 * tokens, cols), jnp.bfloat16),
            pltpu.VMEM((2 * tokens, cols), jnp.bfloat16),
            pltpu.VMEM((steps, 2 * tokens, cols), jnp.bfloat16),
            pltpu.VMEM(out_weight.shape, jnp.bfloat16),
            pltpu.SemaphoreType.DMA,
        ],
        compiler_params=pltpu.CompilerParams(vmem_limit_bytes=VMEM_BYTES),
        name="block",
    )(scale, lat, mod, qkv_weight, qkv_weight, qkv_weight, out_weight, head_weight)


def return_kernel(n_cfg, n_seq, src_ref, out_ref, land, send, recv):
    cfg, me = lax.axis_index("cfg"), lax.axis_index("seq")
    total = n_cfg * n_seq
    mine = cfg * n_seq + me
    frames = out_ref.shape[0]
    items = src_ref.shape[1]

    greet_all(n_cfg, n_seq)

    def copy(k):
        flat = lax.rem(mine + k, total)
        peer = lax.rem(flat, n_seq)
        return pltpu.make_async_remote_copy(
            src_ref=src_ref.at[pl.ds(peer * frames, frames)], dst_ref=land.at[mine],
            send_sem=send.at[k], recv_sem=recv.at[k],
            device_id=(flat // n_seq, peer), device_id_type=MESH,
        )

    def start(k, carry):
        copy(k).start()
        return carry

    def end(k, carry):
        copy(k).wait()
        return carry

    lax.fori_loop(1, total, start, 0)
    land[mine] = src_ref[pl.ds(me * frames, frames)]
    lax.fori_loop(1, total, end, 0)
    for j in range(total):
        out_ref[:, j * items : (j + 1) * items, :] = land[j]


def send_back(n_cfg, n_seq, guided):
    all_frames, items, out_ch = guided.shape
    frames = all_frames // n_seq
    total = n_cfg * n_seq
    vmem = pl.BlockSpec(memory_space=pltpu.VMEM)
    return pl.pallas_call(
        functools.partial(return_kernel, n_cfg, n_seq),
        out_shape=jax.ShapeDtypeStruct((frames, items * total, out_ch), jnp.float32),
        in_specs=[vmem],
        out_specs=vmem,
        scratch_shapes=[
            pltpu.VMEM((total, frames, items, out_ch), jnp.float32),
            pltpu.SemaphoreType.DMA((total,)),
            pltpu.SemaphoreType.DMA((total,)),
        ],
        compiler_params=pltpu.CompilerParams(
            collective_id=1, has_side_effects=True, vmem_limit_bytes=VMEM_BYTES
        ),
        name="send_back",
    )(guided)


def on_device(
    latent, text_ids, timestep, guide_num, guide_den, text_table,
    time_in, time_out, mod_weight, qkv_weight, out_weight, head_weight,
):
    width = latent.shape[2]
    n_cfg, n_seq = lax.axis_size("cfg"), lax.axis_size("seq")
    me = lax.axis_index("seq")
    time_hidden = jax.nn.silu(
        jnp.dot(time_features(timestep), time_in, preferred_element_type=jnp.float32)
    ).astype(jnp.bfloat16)
    time_part = jnp.dot(time_hidden, time_out, preferred_element_type=jnp.float32)
    placed = lax.dynamic_update_slice(
        jnp.zeros((1, width), jnp.float32), time_part, (0, me * time_out.shape[1])
    )
    ids_local = (text_ids[0] - me * text_table.shape[0])[:, None]
    message = pool(ids_local, placed, text_table)
    lat, mods = exchange(n_cfg, n_seq, message, latent, mod_weight)
    mod = jnp.transpose(mods, (1, 0, 2)).reshape(n_cfg, 5, width)
    guide_scale = guide_num[0].astype(jnp.float32) / guide_den[0].astype(jnp.float32)
    guided = block(
        guide_scale.reshape(1, 1), lat, mod, qkv_weight, out_weight, head_weight
    )
    return send_back(n_cfg, n_seq, guided)


def solution(mesh):
    in_specs = (
        P("seq", None, None), P("cfg", None), P(), P(), P(), P("seq", None),
        P(), P(None, "seq"), P(None, "seq"), P(), P(), P(),
    )
    return jax.shard_map(
        on_device, mesh=mesh, in_specs=in_specs, out_specs=P("seq", None, None), check_vma=False
    )
```

```python
import functools
import math

import jax
import jax.numpy as jnp
from jax import lax
from jax.experimental import pallas as pl
from jax.experimental.pallas import tpu as pltpu
from jax.sharding import PartitionSpec as P

HEADS = 24
FREQ = 256
NORM_FLOOR = 0.1
GROUP = 8
VMEM_BYTES = 60 * 1024 * 1024
MESH = pl.DeviceIdType.MESH


def layer_norm(values):
    center = values - jnp.mean(values, axis=-1, keepdims=True)
    spread = jnp.mean(center * center, axis=-1, keepdims=True)
    return center * lax.rsqrt(spread + NORM_FLOOR)


def time_features(timestep):
    half_width = FREQ // 2
    ladder = jnp.arange(half_width, dtype=jnp.float32)
    freq_rates = jnp.exp(-math.log(10000.0) * ladder / half_width)
    angles = timestep.astype(jnp.float32)[0] * freq_rates
    return jnp.concatenate([jnp.cos(angles), jnp.sin(angles)])[None, :].astype(jnp.bfloat16)


def greet_all(n_cfg, n_seq):
    cfg, me = lax.axis_index("cfg"), lax.axis_index("seq")
    barrier = pltpu.get_barrier_semaphore()
    total = n_cfg * n_seq

    def hello(k, carry):
        flat = lax.rem(cfg * n_seq + me + k, total)
        pl.semaphore_signal(
            barrier, inc=1, device_id=(flat // n_seq, lax.rem(flat, n_seq)), device_id_type=MESH
        )
        return carry

    lax.fori_loop(1, total, hello, 0)
    pl.semaphore_wait(barrier, total - 1)


def whole_kernel(
    n_cfg, n_seq, head_dim, scale_ref, ids_ref, placed_ref, latent_ref, table_hbm, mod_w_hbm,
    wqkv_hbm, wo_hbm, wh_hbm, out_ref,
    table, mod_w, wqkv, wo, wh, lat, slots, mods, part, mod_all, normed, qs, ks, vs, mixed, preds,
    load_sem, msg_send, msg_recv, lat_send, lat_recv, mod_send, mod_recv, ret_send, ret_recv,
):
    cfg, me = lax.axis_index("cfg"), lax.axis_index("seq")
    total = n_cfg * n_seq
    mine = cfg * n_seq + me
    frames, pixels, width = latent_ref.shape
    half = pixels // n_cfg
    items = half // n_seq
    groups, all_frames = lat.shape[0], lat.shape[1]
    rows = all_frames * GROUP
    tokens = ids_ref.shape[1]
    voc = table.shape[0]

    loads = []
    for n, (src, dst) in enumerate(
        ((table_hbm, table), (mod_w_hbm, mod_w), (wqkv_hbm, wqkv), (wo_hbm, wo), (wh_hbm, wh))
    ):
        loads.append(pltpu.make_async_copy(src, dst, load_sem.at[n]))
        loads[-1].start()

    def piece(owner, g):
        start = pl.multiple_of(cfg * half + owner * items + g * GROUP, GROUP)
        return latent_ref.at[:, pl.ds(start, GROUP), :]

    def lat_copy(g, k):
        peer = lax.rem(me + k, n_seq)
        return pltpu.make_async_remote_copy(
            src_ref=piece(peer, g), dst_ref=lat.at[g, pl.ds(me * frames, frames)],
            send_sem=lat_send.at[g, k], recv_sem=lat_recv.at[g, k],
            device_id=(cfg, peer), device_id_type=MESH,
        )

    def own_copy(g):
        return pltpu.make_async_copy(
            piece(me, g), lat.at[g, pl.ds(me * frames, frames)], lat_send.at[g, 0]
        )

    def msg_copy(k):
        flat = lax.rem(mine + k, total)
        return pltpu.make_async_remote_copy(
            src_ref=slots.at[mine], dst_ref=slots.at[mine], send_sem=msg_send.at[k],
            recv_sem=msg_recv.at[k],
            device_id=(flat // n_seq, lax.rem(flat, n_seq)), device_id_type=MESH,
        )

    def mod_copy(k):
        peer = lax.rem(me + k, n_seq)
        return pltpu.make_async_remote_copy(
            src_ref=part, dst_ref=mods.at[me], send_sem=mod_send.at[k], recv_sem=mod_recv.at[k],
            device_id=(cfg, peer), device_id_type=MESH,
        )

    def ret_copy(g, k):
        flat = lax.rem(mine + k, total)
        peer = lax.rem(flat, n_seq)
        start = pl.multiple_of(mine * items + g * GROUP, GROUP)
        return pltpu.make_async_remote_copy(
            src_ref=preds.at[g, pl.ds(peer * frames, frames)],
            dst_ref=out_ref.at[:, pl.ds(start, GROUP), :],
            send_sem=ret_send.at[g, k], recv_sem=ret_recv.at[g, k],
            device_id=(flat // n_seq, peer), device_id_type=MESH,
        )

    def own_ret(g):
        start = pl.multiple_of(mine * items + g * GROUP, GROUP)
        return pltpu.make_async_copy(
            preds.at[g, pl.ds(me * frames, frames)],
            out_ref.at[:, pl.ds(start, GROUP), :],
            ret_send.at[g, 0],
        )

    def each(count, act):
        def run(k, carry):
            act(k)
            return carry

        lax.fori_loop(1, count, run, 0)

    greet_all(n_cfg, n_seq)
    own_copy(0).start()
    each(n_seq, lambda k: lat_copy(0, k).start())

    ids = jnp.broadcast_to(ids_ref[...] - me * voc, (128, tokens)).T
    lanes = lax.broadcasted_iota(jnp.int32, (tokens, 128), 1)
    tiles = []
    for t in range(-(-voc // 128)):
        hits = jnp.where(ids == lanes + t * 128, 1.0, 0.0)
        tiles.append(jnp.sum(hits, axis=0, keepdims=True))
    counts = jnp.concatenate(tiles, axis=1)[:, :voc]
    high = jnp.floor(counts * (1.0 / 256.0)) * 256.0
    counts = jnp.concatenate([high, counts - high], axis=0).astype(jnp.bfloat16)
    loads[0].wait()
    sums = jnp.dot(counts, table[...], preferred_element_type=jnp.float32)
    pooled = jnp.sum(sums, axis=0, keepdims=True) * (1.0 / math.sqrt(tokens))
    slots[mine] = pooled + placed_ref[...]
    each(total, lambda k: msg_copy(k).start())
    loads[1].wait()
    each(total, lambda k: msg_copy(k).wait())
    conds = []
    for c in range(n_cfg):
        conds.append(jnp.sum(slots[c * n_seq : (c + 1) * n_seq], axis=0))
    cond = jnp.concatenate(conds, axis=0)
    cond = (cond / (1.0 + jnp.exp(-cond))).astype(jnp.bfloat16)
    mod_part = jnp.dot(cond, mod_w[...], preferred_element_type=jnp.float32)
    part[...] = mod_part
    mods[me] = mod_part
    each(n_seq, lambda k: mod_copy(k).start())
    for g in range(1, groups):
        own_copy(g).start()
        each(n_seq, lambda k: lat_copy(g, k).start())
    each(n_seq, lambda k: mod_copy(k).wait())
    mod_all[...] = jnp.concatenate([mods[s] for s in range(n_seq)], axis=1)
    loads[2].wait()
    loads[3].wait()
    loads[4].wait()

    def modulation(c, n):
        return mod_all[c : c + 1, n * width : (n + 1) * width]

    cols = qs.shape[2]
    steps = width // cols
    pair = 2 * head_dim
    lane = lax.broadcasted_iota(jnp.int32, (1, pair), 1)
    left = jnp.where(lane < head_dim, 1.0, 0.0).astype(jnp.bfloat16)
    right = jnp.where(lane < head_dim, 0.0, 1.0).astype(jnp.bfloat16)
    same = lax.broadcasted_iota(jnp.int32, (1, GROUP, rows), 1) == lax.rem(
        lax.broadcasted_iota(jnp.int32, (1, GROUP, rows), 2), GROUP
    )
    shares = jnp.concatenate(
        [jnp.broadcast_to(left, (rows, pair)), jnp.broadcast_to(right, (rows, pair))], axis=0
    )

    def project(j):
        at = slice(j * cols, (j + 1) * cols)
        x = normed[...]
        q = jnp.dot(x, wqkv[:, at], preferred_element_type=jnp.float32)
        qs[j % 2] = (q * (1.0 / math.sqrt(head_dim))).astype(jnp.bfloat16)
        at = slice(width + j * cols, width + (j + 1) * cols)
        k = jnp.dot(x, wqkv[:, at], preferred_element_type=jnp.float32)
        ks[j % 2] = k.astype(jnp.bfloat16)
        at = slice(2 * width + j * cols, 2 * width + (j + 1) * cols)
        v = jnp.dot(x, wqkv[:, at], preferred_element_type=jnp.float32)
        vs[j % 2] = v.astype(jnp.bfloat16)

    def attend(j, c, h):
        at = slice(c * rows, (c + 1) * rows)
        lanes = slice(h * pair, (h + 1) * pair)
        kk = ks[j % 2, at, lanes]
        vv = vs[j % 2, at, lanes]
        keys = jnp.concatenate([kk * left, kk * right], axis=0)
        vals = jnp.concatenate([vv * left, vv * right], axis=0)
        vals = jnp.concatenate([vals, shares], axis=1)
        scores = lax.dot_general(
            qs[j % 2, at, lanes], keys, (((1,), (1,)), ((), ())),
            preferred_element_type=jnp.float32,
        )
        probs = []
        for s in range(2):
            t = scores[:, s * rows : (s + 1) * rows].reshape(all_frames, GROUP, rows)
            t = jnp.where(same, t, -jnp.inf).reshape(rows, rows)
            e = jnp.exp(t - jnp.max(t, axis=1, keepdims=True))
            probs.append(e.astype(jnp.bfloat16))
        both = jnp.dot(
            jnp.concatenate(probs, axis=1), vals, preferred_element_type=jnp.float32
        )
        o = both[:, :pair] / both[:, pair:]
        start = j * cols + h * pair
        mixed[at, start : start + pair] = o.astype(jnp.bfloat16)

    def wave(g, carry):
        own_copy(g).wait()
        each(n_seq, lambda k: lat_copy(g, k).wait_recv())
        x = lat[g].astype(jnp.float32).reshape(rows, width)
        n = layer_norm(x)
        for c in range(n_cfg):
            y = n * (1.0 + modulation(c, 1)) + modulation(c, 0)
            normed[c * rows : (c + 1) * rows, :] = y.astype(jnp.bfloat16)
        project(0)
        for j in range(steps):
            if j + 1 < steps:
                project(j + 1)
            for c in range(n_cfg):
                for h in range(cols // pair):
                    attend(j, c, h)
        branch = jnp.dot(mixed[...], wo[...], preferred_element_type=jnp.float32)
        x = lat[g].astype(jnp.float32).reshape(rows, width)
        finals = []
        for c in range(n_cfg):
            residual = x + modulation(c, 2) * branch[c * rows : (c + 1) * rows]
            final = layer_norm(residual) * (1.0 + modulation(c, 4)) + modulation(c, 3)
            finals.append(final.astype(jnp.bfloat16))
        both = jnp.dot(
            jnp.concatenate(finals, axis=0), wh[...], preferred_element_type=jnp.float32
        )
        guided = both[rows:] + scale_ref[0, 0] * (both[:rows] - both[rows:])
        preds[g] = guided.reshape(all_frames, GROUP, guided.shape[1])
        own_ret(g).start()
        each(total, lambda k: ret_copy(g, k).start())
        return carry

    lax.fori_loop(0, groups, wave, 0)

    def finish(g, carry):
        each(n_seq, lambda k: lat_copy(g, k).wait_send())
        own_ret(g).wait()
        each(total, lambda k: ret_copy(g, k).wait())
        return carry

    lax.fori_loop(0, groups, finish, 0)


def whole(scale, ids, placed, latent, table, mod_weight, qkv_weight, out_weight, head_weight):
    n_cfg, n_seq = lax.axis_size("cfg"), lax.axis_size("seq")
    frames, pixels, width = latent.shape
    head_dim = width // HEADS
    cols = 4 * head_dim
    items = pixels // n_cfg // n_seq
    groups, all_frames = items // GROUP, frames * n_seq
    rows = all_frames * GROUP
    total = n_cfg * n_seq
    mod_cols = mod_weight.shape[1]
    out_ch = head_weight.shape[1]
    vmem = pl.BlockSpec(memory_space=pltpu.VMEM)
    hbm = pl.BlockSpec(memory_space=pl.ANY)
    bf16 = jnp.bfloat16
    dma = pltpu.SemaphoreType.DMA
    return pl.pallas_call(
        functools.partial(whole_kernel, n_cfg, n_seq, head_dim),
        out_shape=jax.ShapeDtypeStruct((frames, pixels, out_ch), jnp.float32),
        in_specs=[
            pl.BlockSpec(memory_space=pltpu.SMEM), vmem, vmem, hbm, hbm, hbm, hbm, hbm, hbm,
        ],
        out_specs=hbm,
        scratch_shapes=[
            pltpu.VMEM(table.shape, bf16),
            pltpu.VMEM(mod_weight.shape, bf16),
            pltpu.VMEM(qkv_weight.shape, bf16),
            pltpu.VMEM(out_weight.shape, bf16),
            pltpu.VMEM(head_weight.shape, bf16),
            pltpu.VMEM((groups, all_frames, GROUP, width), bf16),
            pltpu.VMEM((total, 1, width), jnp.float32),
            pltpu.VMEM((n_seq, n_cfg, mod_cols), jnp.float32),
            pltpu.VMEM((n_cfg, mod_cols), jnp.float32),
            pltpu.VMEM((n_cfg, n_seq * mod_cols), jnp.float32),
            pltpu.VMEM((n_cfg * rows, width), bf16),
            pltpu.VMEM((2, n_cfg * rows, cols), bf16),
            pltpu.VMEM((2, n_cfg * rows, cols), bf16),
            pltpu.VMEM((2, n_cfg * rows, cols), bf16),
            pltpu.VMEM((n_cfg * rows, width), bf16),
            pltpu.VMEM((groups, all_frames, GROUP, out_ch), jnp.float32),
            dma((5,)),
            dma((total,)), dma((total,)),
            dma((groups, n_seq)), dma((groups, n_seq)),
            dma((n_seq,)), dma((n_seq,)),
            dma((groups, total)), dma((groups, total)),
        ],
        compiler_params=pltpu.CompilerParams(
            collective_id=0, has_side_effects=True, vmem_limit_bytes=VMEM_BYTES
        ),
        name="whole",
    )(scale, ids, placed, latent, table, mod_weight, qkv_weight, out_weight, head_weight)


def on_device(
    latent, text_ids, timestep, guide_num, guide_den, text_table,
    time_in, time_out, mod_weight, qkv_weight, out_weight, head_weight,
):
    width = latent.shape[2]
    me = lax.axis_index("seq")
    time_hidden = jax.nn.silu(
        jnp.dot(time_features(timestep), time_in, preferred_element_type=jnp.float32)
    ).astype(jnp.bfloat16)
    time_part = jnp.dot(time_hidden, time_out, preferred_element_type=jnp.float32)
    placed = lax.dynamic_update_slice(
        jnp.zeros((1, width), jnp.float32), time_part, (0, me * time_out.shape[1])
    )
    guide_scale = guide_num[0].astype(jnp.float32) / guide_den[0].astype(jnp.float32)
    return whole(
        guide_scale.reshape(1, 1), text_ids, placed, latent, text_table, mod_weight,
        qkv_weight, out_weight, head_weight,
    )


def solution(mesh):
    in_specs = (
        P("seq", None, None), P("cfg", None), P(), P(), P(), P("seq", None),
        P(), P(None, "seq"), P(None, "seq"), P(), P(), P(),
    )
    return jax.shard_map(
        on_device, mesh=mesh, in_specs=in_specs, out_specs=P("seq", None, None), check_vma=False
    )
```
